32 devices in a mesh: subj: 16 (over z, y, x), vox: 2 (over core).
Axes of the slice: x: 2, y: 2, z: 4, core: 2. Of those that a mesh axis runs over, the one named last changes fastest.
Arguments:
- bold_series: float32 [16, 300, 16384], P('subj', None, 'vox')
- seed_index: int32 [256], replicated, may hold values from 0 to 16383
Outputs:
- group_z: float32 [16384, 256], P(('vox', 'subj'))
The draws below stay inside these ranges and needn't reach their ends.
All inputs are finite; a program needn't handle non-finite values.
Results may differ from the reference program's by a relative error of at most 0.00031.
Values may be sent and summed in bfloat16 or wider, within the bound.
A program may use at most 64 MiB of HBM per device.

```python
import math
import jax
import jax.numpy as jnp
from jax import lax

TIMEPOINTS = 300
SEEDS = 256
SUBJ = 16
VOXELS = 16384


def draw_bold_series(key, part):
    factors = 4
    subkeys = jax.random.split(key, 6)
    hidden_factors = jax.random.normal(subkeys[0], (SUBJ, factors, TIMEPOINTS), jnp.float32)
    common_component = jax.random.normal(subkeys[1], (factors, VOXELS), jnp.float32) * (0.8 / math.sqrt(factors))
    subject_specific = jax.random.normal(subkeys[2], (SUBJ, factors, VOXELS), jnp.float32) * (0.6 / math.sqrt(factors))
    signal_component = jnp.einsum('oju,ojf->ouf', hidden_factors, common_component[None] + subject_specific)
    noise_part = jax.random.normal(subkeys[3], (SUBJ, TIMEPOINTS, VOXELS), jnp.float32)
    scale_factors = jnp.exp(jax.random.uniform(subkeys[4], (SUBJ, 1, VOXELS), jnp.float32, 0.0, math.log(10.0)))
    offsets = jax.random.uniform(subkeys[5], (SUBJ, 1, VOXELS), jnp.float32, -5.0, 5.0)
    return offsets + scale_factors * (signal_component + noise_part)


def place_ends(drawn, rng, smallest, largest):
    longest = drawn.shape.index(max(drawn.shape))
    spots = []
    for shift in (0, 1):
        where = [jax.random.randint(jax.random.fold_in(rng, axis), (), 0, length) for axis, length in enumerate(drawn.shape)]
        where[longest] = (where[longest] + shift) % drawn.shape[longest]
        spots.append(tuple(where))
    return drawn.at[spots[0]].set(smallest).at[spots[1]].set(largest)


def setup_inputs(seed: int = 0) -> dict:
    arg_keys = jax.random.split(jax.random.key(seed), 3)
    return {
        "bold_series": draw_bold_series(jax.random.fold_in(arg_keys[2], 71), 0),
        "seed_index": place_ends(jax.random.randint(arg_keys[1], (SEEDS,), 0, VOXELS), jax.random.fold_in(arg_keys[1], 1), 0, VOXELS - 1).astype(jnp.int32),
    }


clip_limit = 0.99
epsilon = 1e-05

def normalize(series):
    demean_series = series - lax.optimization_barrier(jnp.mean(series, axis=0, keepdims=True))
    spread = lax.optimization_barrier(jnp.mean(demean_series * demean_series, axis=0, keepdims=True))
    return (demean_series * lax.rsqrt(spread + epsilon)).astype(jnp.bfloat16)

def arctanh_transform(cross_product, length):
    clipped = jnp.clip(cross_product * (1.0 / length), -clip_limit, clip_limit)
    return 0.5 * jnp.log((1.0 + clipped) / (1.0 - clipped))

def reference(bold_series, seed_index):
    length = bold_series.shape[1]

    def accumulate(summed, series):
        normed = normalize(series)
        seed_panel = jnp.take(normed, seed_index.astype(jnp.int32), axis=1)
        cross_product = lax.dot_general(normed, seed_panel, (((0,), (0,)), ((), ())), preferred_element_type=jnp.float32)
        return (summed + arctanh_transform(cross_product, length), None)
    start_sum = jnp.zeros((bold_series.shape[2], seed_index.shape[0]), jnp.float32)
    summed, unused = lax.scan(accumulate, start_sum, bold_series)
    return summed * (1.0 / SUBJ)
```

```python
import functools
import math

import jax
import jax.numpy as jnp
from jax import lax
from jax.experimental import pallas as pl
from jax.experimental.pallas import tpu as pltpu
from jax.sharding import PartitionSpec as P

clip_limit = 0.99
epsilon = 1e-05
MESH = pl.DeviceIdType.MESH
z_limit = 0.5 * math.log((1.0 + clip_limit) / (1.0 - clip_limit))
code_top = 32700.0


def encode(value, terms):
    scale = code_top / math.sqrt(terms * z_limit)
    root = value * lax.rsqrt(jnp.maximum(jnp.abs(value), 1e-30))
    return jnp.round(root * scale).astype(jnp.int32).astype(jnp.int16)


def decode(code, terms):
    scale = math.sqrt(terms * z_limit) / code_top
    root = code.astype(jnp.int32).astype(jnp.float32) * scale
    return root * jnp.abs(root)


def kernel(n, nv, chunk, bold, seeds, out, raw, norm, acc, pan_out, pan_in, pan_t,
           s1_out, s1_in, s2_out, s2_in, s3_out, s3_in,
           load_sem, p_send, p_recv, a_send, a_recv, b_send, b_recv, c_send, c_recv):
    length, columns = raw.shape
    block = columns // n
    hi_count = n // 4
    s = lax.axis_index("subj")
    v = lax.axis_index("vox")
    odd = lax.rem(v, 2)
    w1, w2 = 1 + odd, 2 - odd
    f, g = lax.rem(s // w1, 2), lax.rem(s // w2, 2)
    hi, lo = s // 4, lax.rem(s, 4)
    mate1 = s + w1 * (1 - 2 * f)
    mate2 = s + w2 * (1 - 2 * g)

    loads = columns // chunk

    def load(i):
        cols = pl.ds(pl.multiple_of(i * chunk, 128), chunk)
        return pltpu.make_async_copy(bold.at[0, :, cols], raw.at[:, cols], load_sem.at[i])

    for i in range(loads):
        load(i).start()

    barrier = pltpu.get_barrier_semaphore()
    pl.semaphore_signal(barrier, inc=1, device_id={"subj": mate1}, device_id_type=MESH)
    pl.semaphore_signal(barrier, inc=1, device_id={"subj": mate2}, device_id_type=MESH)
    for j in range(1, hi_count):
        peer = lax.rem(hi + j, hi_count) * 4 + lo
        pl.semaphore_signal(barrier, inc=1, device_id={"subj": peer}, device_id_type=MESH)
    for j in range(1, nv):
        pl.semaphore_signal(
            barrier, inc=1, device_id={"vox": lax.rem(v + j, nv)}, device_id_type=MESH
        )

    acc[...] = jnp.zeros_like(acc)
    wide = 256

    @pl.loop(0, loads)
    def _(i):
        load(i).wait()
        for j in range(chunk // wide):
            cols = pl.ds(pl.multiple_of(i * chunk + j * wide, 128), wide)
            x = raw[:, cols]
            x = x - jnp.sum(x, axis=0, keepdims=True) * (1.0 / length)
            spread = jnp.sum(x * x, axis=0, keepdims=True) * (1.0 / length)
            norm[:, cols] = (x * lax.rsqrt(spread + epsilon)).astype(jnp.bfloat16)
        cols = pl.ds(pl.multiple_of(i * chunk, 128), chunk)
        rows = lax.broadcasted_iota(jnp.int32, (chunk, seeds.shape[1]), 0)
        hit = rows == seeds[...] - (v * columns + i * chunk)
        pick = jnp.where(hit, 1.0, 0.0).astype(jnp.bfloat16)
        acc[pl.ds(0, length), :] += jnp.dot(
            norm[:, cols], pick, preferred_element_type=jnp.float32
        )

    pl.semaphore_wait(barrier, 2 + (hi_count - 1) + (nv - 1))
    pan_out[...] = acc[pl.ds(0, length), :].astype(jnp.bfloat16)

    def panel_copy(j):
        return pltpu.make_async_remote_copy(
            src_ref=pan_out, dst_ref=pan_in.at[j - 1],
            send_sem=p_send.at[j - 1], recv_sem=p_recv.at[j - 1],
            device_id={"vox": lax.rem(v + j, nv)}, device_id_type=MESH,
        )

    for j in range(1, nv):
        panel_copy(j).start()
    for j in range(1, nv):
        panel_copy(j).wait_recv()
        acc[pl.ds(0, length), :] += pan_in[j - 1].astype(jnp.float32)
    pan_t[...] = acc[...].T.astype(jnp.bfloat16)

    def fisher(step, gg, ff):
        target = lax.rem(hi + hi_count - 1 - step, hi_count)
        start = (target * 4 + gg * w2 + ff * w1) * block
        cols = pl.ds(pl.multiple_of(start, 128), block)
        cross = jnp.dot(
            pan_t[:, pl.ds(0, length)], norm[:, cols], preferred_element_type=jnp.float32
        )
        c = jnp.clip(cross * (1.0 / length), -clip_limit, clip_limit)
        return 0.5 * (jnp.log(1.0 + c) - jnp.log(1.0 - c))

    def copy1(k):
        return pltpu.make_async_remote_copy(
            src_ref=s1_out.at[k], dst_ref=s1_in.at[k], send_sem=a_send.at[k],
            recv_sem=a_recv.at[k], device_id={"subj": mate1}, device_id_type=MESH,
        )

    def copy2(k):
        return pltpu.make_async_remote_copy(
            src_ref=s2_out.at[k], dst_ref=s2_in.at[k], send_sem=b_send.at[k],
            recv_sem=b_recv.at[k], device_id={"subj": mate2}, device_id_type=MESH,
        )

    def copy3(k):
        target = lax.rem(hi + hi_count - 1 - k, hi_count) * 4 + lo
        return pltpu.make_async_remote_copy(
            src_ref=s3_out.at[k], dst_ref=s3_in.at[k], send_sem=c_send.at[k],
            recv_sem=c_recv.at[k], device_id={"subj": target}, device_id_type=MESH,
        )

    @pl.loop(0, hi_count + 2)
    def _(turn):
        @pl.when(turn < hi_count)
        def _():
            s1_out[2 * turn] = encode(fisher(turn, 1 - g, 1 - f), 1)
            copy1(2 * turn).start()
            s1_out[2 * turn + 1] = encode(fisher(turn, g, 1 - f), 1)
            copy1(2 * turn + 1).start()

        @pl.when((turn >= 1) & (turn <= hi_count))
        def _():
            k = turn - 1
            mine = fisher(k, 1 - g, f)
            copy1(2 * k).wait_recv()
            s2_out[k] = encode(mine + decode(s1_in[2 * k], 1), 2)
            copy2(k).start()

        @pl.when(turn >= 2)
        def _():
            k = turn - 2
            mine = fisher(k, g, f)
            copy1(2 * k + 1).wait_recv()
            mine = mine + decode(s1_in[2 * k + 1], 1)
            copy2(k).wait_recv()
            mine = mine + decode(s2_in[k], 2)

            @pl.when(k < hi_count - 1)
            def _():
                s3_out[k] = encode(mine, 4)
                copy3(k).start()

            @pl.when(k == hi_count - 1)
            def _():
                out[...] = mine

    for k in range(hi_count - 1):
        copy3(k).wait_recv()
        out[...] += decode(s3_in[k], 4)
    out[...] = out[...] * (1.0 / n)

    for j in range(1, nv):
        panel_copy(j).wait_send()

    @pl.loop(0, 2 * hi_count)
    def _(k):
        copy1(k).wait_send()

    @pl.loop(0, hi_count)
    def _(k):
        copy2(k).wait_send()

    @pl.loop(0, hi_count - 1)
    def _(k):
        copy3(k).wait_send()


def body(n, nv, bold_series, seed_index):
    _, length, columns = bold_series.shape
    count = seed_index.shape[0]
    block = columns // n
    hi_count = n // 4
    padded = -(-length // 128) * 128
    chunk = 1024 if columns % 1024 == 0 else 256
    i16 = jnp.int16
    dma = pltpu.SemaphoreType.DMA
    result = pl.pallas_call(
        functools.partial(kernel, n, nv, chunk),
        out_shape=jax.ShapeDtypeStruct((count, block), jnp.float32),
        in_specs=[pl.BlockSpec(memory_space=pl.ANY), pl.BlockSpec(memory_space=pltpu.VMEM)],
        out_specs=pl.BlockSpec(memory_space=pltpu.VMEM),
        scratch_shapes=[
            pltpu.VMEM((length, columns), jnp.float32),
            pltpu.VMEM((length, columns), jnp.bfloat16),
            pltpu.VMEM((padded, count), jnp.float32),
            pltpu.VMEM((length, count), jnp.bfloat16),
            pltpu.VMEM((nv - 1, length, count), jnp.bfloat16),
            pltpu.VMEM((count, padded), jnp.bfloat16),
            pltpu.VMEM((2 * hi_count, count, block), i16),
            pltpu.VMEM((2 * hi_count, count, block), i16),
            pltpu.VMEM((hi_count, count, block), i16),
            pltpu.VMEM((hi_count, count, block), i16),
            pltpu.VMEM((hi_count - 1, count, block), i16),
            pltpu.VMEM((hi_count - 1, count, block), i16),
            dma((columns // chunk,)),
            dma((nv - 1,)), dma((nv - 1,)),
            dma((2 * hi_count,)), dma((2 * hi_count,)),
            dma((hi_count,)), dma((hi_count,)),
            dma((hi_count - 1,)), dma((hi_count - 1,)),
        ],
        compiler_params=pltpu.CompilerParams(
            collective_id=0, has_side_effects=True, vmem_limit_bytes=60000 * 1024
        ),
    )(bold_series, seed_index[None, :])
    return result.T


def solution(mesh):
    n, nv = mesh.shape["subj"], mesh.shape["vox"]
    in_specs = (P("subj", None, "vox"), P())
    out_specs = P(("vox", "subj"), None)
    return jax.shard_map(
        functools.partial(body, n, nv), mesh=mesh, in_specs=in_specs, out_specs=out_specs,
        check_vma=False,
    )
```

```python
import functools
import math

import jax
import jax.numpy as jnp
from jax import lax
from jax.experimental import pallas as pl
from jax.experimental.pallas import tpu as pltpu
from jax.sharding import PartitionSpec as P

clip_limit = 0.99
epsilon = 1e-05
MESH = pl.DeviceIdType.MESH
z_limit = 0.5 * math.log((1.0 + clip_limit) / (1.0 - clip_limit))
code_top = 32700.0


def encode(value, terms):
    scale = code_top / math.sqrt(terms * z_limit)
    root = value * lax.rsqrt(jnp.maximum(jnp.abs(value), 1e-30))
    return jnp.round(root * scale).astype(jnp.int32).astype(jnp.int16)


def decode(code, terms):
    scale = math.sqrt(terms * z_limit) / code_top
    root = code.astype(jnp.int32).astype(jnp.float32) * scale
    return root * jnp.abs(root)


def kernel(n, nv, chunk, bold, seeds, out, raw, norm, acc, pan_out, pan_in, pan_t,
           s1_out, s1_in, s2_out, s2_in, s3_out, s3_in,
           load_sem, p_send, p_recv, a_send, a_recv, b_send, b_recv, c_send, c_recv):
    length, columns = norm.shape
    block = columns // n
    hi_count = n // 4
    s = lax.axis_index("subj")
    v = lax.axis_index("vox")
    odd = lax.rem(v, 2)
    w1, w2 = 1 + odd, 2 - odd
    f, g = lax.rem(s // w1, 2), lax.rem(s // w2, 2)
    hi, lo = s // 4, lax.rem(s, 4)
    mate1 = s + w1 * (1 - 2 * f)
    mate2 = s + w2 * (1 - 2 * g)

    loads, lines = columns // chunk, chunk // 128

    def load(i):
        tiles = pl.ds(pl.multiple_of(i * lines, 8), lines)
        return pltpu.make_async_copy(
            bold.at[:, tiles, :], raw.at[i].reshape(length, lines, 128), load_sem.at[i]
        )

    for i in range(loads):
        load(i).start()

    barrier = pltpu.get_barrier_semaphore()
    pl.semaphore_signal(barrier, inc=1, device_id={"subj": mate1}, device_id_type=MESH)
    pl.semaphore_signal(barrier, inc=1, device_id={"subj": mate2}, device_id_type=MESH)
    for j in range(1, hi_count):
        peer = lax.rem(hi + j, hi_count) * 4 + lo
        pl.semaphore_signal(barrier, inc=1, device_id={"subj": peer}, device_id_type=MESH)
    for j in range(1, nv):
        pl.semaphore_signal(
            barrier, inc=1, device_id={"vox": lax.rem(v + j, nv)}, device_id_type=MESH
        )

    acc[...] = jnp.zeros_like(acc)

    @pl.loop(0, loads)
    def _(i):
        load(i).wait()
        for j in range(lines):
            cols = pl.ds(pl.multiple_of(i * chunk + j * 128, 128), 128)
            x = raw[i, pl.ds(j, length, stride=lines), :]
            x = x - jnp.sum(x, axis=0, keepdims=True) * (1.0 / length)
            spread = jnp.sum(x * x, axis=0, keepdims=True) * (1.0 / length)
            norm[:, cols] = (x * lax.rsqrt(spread + epsilon)).astype(jnp.bfloat16)
        cols = pl.ds(pl.multiple_of(i * chunk, 128), chunk)
        rows = lax.broadcasted_iota(jnp.int32, (chunk, seeds.shape[1]), 0)
        hit = rows == seeds[...] - (v * columns + i * chunk)
        pick = jnp.where(hit, 1.0, 0.0).astype(jnp.bfloat16)
        acc[pl.ds(0, length), :] += jnp.dot(
            norm[:, cols], pick, preferred_element_type=jnp.float32
        )

    pl.semaphore_wait(barrier, 2 + (hi_count - 1) + (nv - 1))
    pan_out[...] = acc[pl.ds(0, length), :].astype(jnp.bfloat16)

    def panel_copy(j):
        return pltpu.make_async_remote_copy(
            src_ref=pan_out, dst_ref=pan_in.at[j - 1],
            send_sem=p_send.at[j - 1], recv_sem=p_recv.at[j - 1],
            device_id={"vox": lax.rem(v + j, nv)}, device_id_type=MESH,
        )

    for j in range(1, nv):
        panel_copy(j).start()
    for j in range(1, nv):
        panel_copy(j).wait_recv()
        acc[pl.ds(0, length), :] += pan_in[j - 1].astype(jnp.float32)
    pan_t[...] = acc[...].T.astype(jnp.bfloat16)

    def fisher(step, gg, ff):
        target = lax.rem(hi + hi_count - 1 - step, hi_count)
        start = (target * 4 + gg * w2 + ff * w1) * block
        cols = pl.ds(pl.multiple_of(start, 128), block)
        cross = jnp.dot(
            pan_t[:, pl.ds(0, length)], norm[:, cols], preferred_element_type=jnp.float32
        )
        c = jnp.clip(cross * (1.0 / length), -clip_limit, clip_limit)
        return 0.5 * (jnp.log(1.0 + c) - jnp.log(1.0 - c))

    def copy1(k):
        return pltpu.make_async_remote_copy(
            src_ref=s1_out.at[k], dst_ref=s1_in.at[k], send_sem=a_send.at[k],
            recv_sem=a_recv.at[k], device_id={"subj": mate1}, device_id_type=MESH,
        )

    def copy2(k):
        return pltpu.make_async_remote_copy(
            src_ref=s2_out.at[k], dst_ref=s2_in.at[k], send_sem=b_send.at[k],
            recv_sem=b_recv.at[k], device_id={"subj": mate2}, device_id_type=MESH,
        )

    def copy3(k):
        target = lax.rem(hi + hi_count - 1 - k, hi_count) * 4 + lo
        return pltpu.make_async_remote_copy(
            src_ref=s3_out.at[k], dst_ref=s3_in.at[k], send_sem=c_send.at[k],
            recv_sem=c_recv.at[k], device_id={"subj": target}, device_id_type=MESH,
        )

    @pl.loop(0, hi_count + 2)
    def _(turn):
        @pl.when(turn < hi_count)
        def _():
            s1_out[2 * turn] = encode(fisher(turn, 1 - g, 1 - f), 1)
            copy1(2 * turn).start()
            s1_out[2 * turn + 1] = encode(fisher(turn, g, 1 - f), 1)
            copy1(2 * turn + 1).start()

        @pl.when((turn >= 1) & (turn <= hi_count))
        def _():
            k = turn - 1
            mine = fisher(k, 1 - g, f)
            copy1(2 * k).wait_recv()
            s2_out[k] = encode(mine + decode(s1_in[2 * k], 1), 2)
            copy2(k).start()

        @pl.when(turn >= 2)
        def _():
            k = turn - 2
            mine = fisher(k, g, f)
            copy1(2 * k + 1).wait_recv()
            mine = mine + decode(s1_in[2 * k + 1], 1)
            copy2(k).wait_recv()
            mine = mine + decode(s2_in[k], 2)

            @pl.when(k < hi_count - 1)
            def _():
                s3_out[k] = encode(mine, 4)
                copy3(k).start()

            @pl.when(k == hi_count - 1)
            def _():
                out[...] = mine

    for k in range(hi_count - 1):
        copy3(k).wait_recv()
        out[...] += decode(s3_in[k], 4)
    out[...] = out[...] * (1.0 / n)

    for j in range(1, nv):
        panel_copy(j).wait_send()

    @pl.loop(0, 2 * hi_count)
    def _(k):
        copy1(k).wait_send()

    @pl.loop(0, hi_count)
    def _(k):
        copy2(k).wait_send()

    @pl.loop(0, hi_count - 1)
    def _(k):
        copy3(k).wait_send()


def body(n, nv, bold_series, seed_index):
    _, length, columns = bold_series.shape
    count = seed_index.shape[0]
    block = columns // n
    hi_count = n // 4
    padded = -(-length // 128) * 128
    chunk = 1024
    i16 = jnp.int16
    dma = pltpu.SemaphoreType.DMA
    result = pl.pallas_call(
        functools.partial(kernel, n, nv, chunk),
        out_shape=jax.ShapeDtypeStruct((count, block), jnp.float32),
        in_specs=[pl.BlockSpec(memory_space=pl.ANY), pl.BlockSpec(memory_space=pltpu.VMEM)],
        out_specs=pl.BlockSpec(memory_space=pltpu.VMEM),
        scratch_shapes=[
            pltpu.VMEM((columns // chunk, length * chunk // 128, 128), jnp.float32),
            pltpu.VMEM((length, columns), jnp.bfloat16),
            pltpu.VMEM((padded, count), jnp.float32),
            pltpu.VMEM((length, count), jnp.bfloat16),
            pltpu.VMEM((nv - 1, length, count), jnp.bfloat16),
            pltpu.VMEM((count, padded), jnp.bfloat16),
            pltpu.VMEM((2 * hi_count, count, block), i16),
            pltpu.VMEM((2 * hi_count, count, block), i16),
            pltpu.VMEM((hi_count, count, block), i16),
            pltpu.VMEM((hi_count, count, block), i16),
            pltpu.VMEM((hi_count - 1, count, block), i16),
            pltpu.VMEM((hi_count - 1, count, block), i16),
            dma((columns // chunk,)),
            dma((nv - 1,)), dma((nv - 1,)),
            dma((2 * hi_count,)), dma((2 * hi_count,)),
            dma((hi_count,)), dma((hi_count,)),
            dma((hi_count - 1,)), dma((hi_count - 1,)),
        ],
        compiler_params=pltpu.CompilerParams(
            collective_id=0, has_side_effects=True, vmem_limit_bytes=60000 * 1024
        ),
    )(bold_series.reshape(length, columns // 128, 128), seed_index[None, :])
    return result.T


def solution(mesh):
    n, nv = mesh.shape["subj"], mesh.shape["vox"]
    in_specs = (P("subj", None, "vox"), P())
    out_specs = P(("vox", "subj"), None)
    return jax.shard_map(
        functools.partial(body, n, nv), mesh=mesh, in_specs=in_specs, out_specs=out_specs,
        check_vma=False,
    )
```

```python
import functools
import math

import jax
import jax.numpy as jnp
from jax import lax
from jax.experimental import pallas as pl
from jax.experimental.pallas import tpu as pltpu
from jax.sharding import PartitionSpec as P

clip_limit = 0.99
epsilon = 1e-05
MESH = pl.DeviceIdType.MESH
z_limit = 0.5 * math.log((1.0 + clip_limit) / (1.0 - clip_limit))
code_top = 32700.0
pieces = 2
ahead = 2


def encode(value, terms):
    scale = code_top / math.sqrt(terms * z_limit)
    root = value * lax.rsqrt(jnp.maximum(jnp.abs(value), 1e-30))
    return jnp.round(root * scale).astype(jnp.int32).astype(jnp.int16)


def decode(code, terms):
    scale = math.sqrt(terms * z_limit) / code_top
    root = code.astype(jnp.int32).astype(jnp.float32) * scale
    return root * jnp.abs(root)


def kernel(n, nv, chunk, bold, seeds, out, raw, norm, acc, pan_out, pan_in, pan_t,
           s1_out, s1_in, s2_out, s2_in, s3_out, s3_in,
           load_sem, p_send, p_recv, a_send, a_recv, b_send, b_recv, c_send, c_recv):
    length, columns = norm.shape
    block = columns // n
    hi_count = n // 4
    steps = hi_count * pieces
    width = block // pieces
    offsets = sorted(range(hi_count), key=lambda d: -min(d, hi_count - d))
    s = lax.axis_index("subj")
    v = lax.axis_index("vox")
    odd = lax.rem(v, 2)
    w1, w2 = 1 + odd, 2 - odd
    f, g = lax.rem(s // w1, 2), lax.rem(s // w2, 2)
    hi, lo = s // 4, lax.rem(s, 4)
    mate1 = s + w1 * (1 - 2 * f)
    mate2 = s + w2 * (1 - 2 * g)

    loads, lines = columns // chunk, chunk // 128

    def load(i):
        tiles = pl.ds(pl.multiple_of(i * lines, 8), lines)
        return pltpu.make_async_copy(
            bold.at[:, tiles, :], raw.at[i].reshape(length, lines, 128), load_sem.at[i]
        )

    for i in range(loads):
        load(i).start()

    barrier = pltpu.get_barrier_semaphore()
    pl.semaphore_signal(barrier, inc=1, device_id={"subj": mate1}, device_id_type=MESH)
    pl.semaphore_signal(barrier, inc=1, device_id={"subj": mate2}, device_id_type=MESH)
    for j in range(1, hi_count):
        peer = lax.rem(hi + j, hi_count) * 4 + lo
        pl.semaphore_signal(barrier, inc=1, device_id={"subj": peer}, device_id_type=MESH)
    for j in range(1, nv):
        pl.semaphore_signal(
            barrier, inc=1, device_id={"vox": lax.rem(v + j, nv)}, device_id_type=MESH
        )

    acc[...] = jnp.zeros_like(acc)

    def normalize(i):
        load(i).wait()
        for j in range(lines):
            cols = pl.ds(pl.multiple_of(i * chunk + j * 128, 128), 128)
            x = raw[i, pl.ds(j, length, stride=lines), :]
            x = x - jnp.sum(x, axis=0, keepdims=True) * (1.0 / length)
            spread = jnp.sum(x * x, axis=0, keepdims=True) * (1.0 / length)
            norm[:, cols] = (x * lax.rsqrt(spread + epsilon)).astype(jnp.bfloat16)

    def pick(i):
        cols = pl.ds(pl.multiple_of(i * chunk, 128), chunk)
        rows = lax.broadcasted_iota(jnp.int32, (chunk, seeds.shape[1]), 0)
        hit = rows == seeds[...] - (v * columns + i * chunk)
        acc[pl.ds(0, length), :] += jnp.dot(
            norm[:, cols], jnp.where(hit, 1.0, 0.0).astype(jnp.bfloat16),
            preferred_element_type=jnp.float32,
        )

    normalize(0)

    @pl.loop(1, loads)
    def _(i):
        pick(i - 1)
        normalize(i)

    pick(loads - 1)

    pl.semaphore_wait(barrier, 2 + (hi_count - 1) + (nv - 1))
    pan_out[...] = acc[pl.ds(0, length), :].astype(jnp.bfloat16)

    def panel_copy(j):
        return pltpu.make_async_remote_copy(
            src_ref=pan_out, dst_ref=pan_in.at[j - 1],
            send_sem=p_send.at[j - 1], recv_sem=p_recv.at[j - 1],
            device_id={"vox": lax.rem(v + j, nv)}, device_id_type=MESH,
        )

    for j in range(1, nv):
        panel_copy(j).start()
    for j in range(1, nv):
        panel_copy(j).wait_recv()
        acc[pl.ds(0, length), :] += pan_in[j - 1].astype(jnp.float32)
    pan_t[...] = acc[...].T.astype(jnp.bfloat16)

    def target_of(step):
        turn = step // pieces
        offset = 0
        for place, d in enumerate(offsets):
            offset = offset + jnp.where(turn == place, d, 0)
        return lax.rem(hi + offset, hi_count)

    def fisher(step, gg, ff):
        start = (target_of(step) * 4 + gg * w2 + ff * w1) * block
        start = start + lax.rem(step, pieces) * width
        cols = pl.ds(pl.multiple_of(start, 128), width)
        cross = jnp.dot(
            pan_t[:, pl.ds(0, length)], norm[:, cols], preferred_element_type=jnp.float32
        )
        c = jnp.clip(cross * (1.0 / length), -clip_limit, clip_limit)
        return 0.5 * (jnp.log(1.0 + c) - jnp.log(1.0 - c))

    def copy1(k):
        return pltpu.make_async_remote_copy(
            src_ref=s1_out.at[k], dst_ref=s1_in.at[k], send_sem=a_send.at[k],
            recv_sem=a_recv.at[k], device_id={"subj": mate1}, device_id_type=MESH,
        )

    def copy2(k):
        return pltpu.make_async_remote_copy(
            src_ref=s2_out.at[k], dst_ref=s2_in.at[k], send_sem=b_send.at[k],
            recv_sem=b_recv.at[k], device_id={"subj": mate2}, device_id_type=MESH,
        )

    def copy3(k):
        target = target_of(k) * 4 + lo
        return pltpu.make_async_remote_copy(
            src_ref=s3_out.at[k], dst_ref=s3_in.at[k], send_sem=c_send.at[k],
            recv_sem=c_recv.at[k], device_id={"subj": target}, device_id_type=MESH,
        )

    @pl.loop(0, steps + ahead + 1)
    def _(turn):
        @pl.when(turn < steps)
        def _():
            s1_out[2 * turn] = encode(fisher(turn, 1 - g, 1 - f), 1)
            copy1(2 * turn).start()
            s1_out[2 * turn + 1] = encode(fisher(turn, g, 1 - f), 1)
            copy1(2 * turn + 1).start()

        @pl.when((turn >= ahead) & (turn < steps + ahead))
        def _():
            k = turn - ahead
            mine = fisher(k, 1 - g, f)
            copy1(2 * k).wait_recv()
            s2_out[k] = encode(mine + decode(s1_in[2 * k], 1), 2)
            copy2(k).start()

        @pl.when(turn >= ahead + 1)
        def _():
            k = turn - ahead - 1
            mine = fisher(k, g, f)
            copy1(2 * k + 1).wait_recv()
            mine = mine + decode(s1_in[2 * k + 1], 1)
            copy2(k).wait_recv()
            mine = mine + decode(s2_in[k], 2)

            @pl.when(k < steps - pieces)
            def _():
                s3_out[k] = encode(mine, 4)
                copy3(k).start()

            @pl.when(k >= steps - pieces)
            def _():
                cols = pl.ds(pl.multiple_of((k - steps + pieces) * width, 128), width)
                out[:, cols] = mine

    for p in range(pieces):
        cols = pl.ds(p * width, width)
        for k in range(p, steps - pieces, pieces):
            copy3(k).wait_recv()
        total = out[:, cols]
        for k in range(p, steps - pieces, pieces):
            total = total + decode(s3_in[k], 4)
        out[:, cols] = total * (1.0 / n)

    for j in range(1, nv):
        panel_copy(j).wait_send()

    @pl.loop(0, 2 * steps)
    def _(k):
        copy1(k).wait_send()

    @pl.loop(0, steps)
    def _(k):
        copy2(k).wait_send()

    @pl.loop(0, steps - pieces)
    def _(k):
        copy3(k).wait_send()


def body(n, nv, bold_series, seed_index):
    _, length, columns = bold_series.shape
    count = seed_index.shape[0]
    block = columns // n
    steps = n // 4 * pieces
    width = block // pieces
    padded = -(-length // 128) * 128
    chunk = 1024
    i16 = jnp.int16
    dma = pltpu.SemaphoreType.DMA
    result = pl.pallas_call(
        functools.partial(kernel, n, nv, chunk),
        out_shape=jax.ShapeDtypeStruct((count, block), jnp.float32),
        in_specs=[pl.BlockSpec(memory_space=pl.ANY), pl.BlockSpec(memory_space=pltpu.VMEM)],
        out_specs=pl.BlockSpec(memory_space=pltpu.VMEM),
        scratch_shapes=[
            pltpu.VMEM((columns // chunk, length * chunk // 128, 128), jnp.float32),
            pltpu.VMEM((length, columns), jnp.bfloat16),
            pltpu.VMEM((padded, count), jnp.float32),
            pltpu.VMEM((length, count), jnp.bfloat16),
            pltpu.VMEM((nv - 1, length, count), jnp.bfloat16),
            pltpu.VMEM((count, padded), jnp.bfloat16),
            pltpu.VMEM((2 * steps, count, width), i16),
            pltpu.VMEM((2 * steps, count, width), i16),
            pltpu.VMEM((steps, count, width), i16),
            pltpu.VMEM((steps, count, width), i16),
            pltpu.VMEM((steps - pieces, count, width), i16),
            pltpu.VMEM((steps - pieces, count, width), i16),
            dma((columns // chunk,)),
            dma((nv - 1,)), dma((nv - 1,)),
            dma((2 * steps,)), dma((2 * steps,)),
            dma((steps,)), dma((steps,)),
            dma((steps - pieces,)), dma((steps - pieces,)),
        ],
        compiler_params=pltpu.CompilerParams(
            collective_id=0, has_side_effects=True, vmem_limit_bytes=60000 * 1024
        ),
    )(bold_series.reshape(length, columns // 128, 128), seed_index[None, :])
    return result.T


def solution(mesh):
    n, nv = mesh.shape["subj"], mesh.shape["vox"]
    in_specs = (P("subj", None, "vox"), P())
    out_specs = P(("vox", "subj"), None)
    return jax.shard_map(
        functools.partial(body, n, nv), mesh=mesh, in_specs=in_specs, out_specs=out_specs,
        check_vma=False,
    )
```
